32 devices in a mesh: pipe: 2 (over x), expert: 8 (over z, core), dp: 2 (over y).
Axes of the slice: x: 2, y: 2, z: 4, core: 2. Of those that a mesh axis runs over, the one named last changes fastest.
Arguments:
- tokens: bfloat16 [2, 2048, 2048], P('pipe', ('expert', 'dp')), may hold values from -6 to 6
- cotangent: bfloat16 [2, 2048, 2048], P('pipe', ('expert', 'dp')), may hold values from -6 to 6
- norm_gain: float32 [2, 2048], P('pipe'), may hold values from 0.5 to 1.5
- first_ids: int32 [2, 2048, 2], P('pipe', ('expert', 'dp')), may hold values from 0 to 3, all different within a row; in each aligned block of 128 rows (0 to 127, 128 to 255, ..., all dimensions but the last counted through in order) at most 72 rows name the same one
- first_gates: float32 [2, 2048, 2], P('pipe', ('expert', 'dp')), may hold values from 0.1 to 1
- second_ids: int32 [2, 2048, 2], P('pipe', ('expert', 'dp')), may hold values from 0 to 3, all different within a row; in each aligned block of 128 rows (0 to 127, 128 to 255, ..., all dimensions but the last counted through in order) at most 72 rows name the same one
- second_gates: float32 [2, 2048, 2], P('pipe', ('expert', 'dp')), may hold values from 0.1 to 1
- new_slot: int32 [2, 4], P('pipe'), may hold values from 0 to 3, each once within a row
- inner_weight: float32 [2, 8, 2, 2048, 384], P('pipe', 'expert', None, 'dp'), may hold values from -0.125 to 0.125
- outer_weight: float32 [2, 8, 384, 2048], P('pipe', 'expert', None, 'dp'), may hold values from -0.21875 to 0.21875
- inner_mean: bfloat16 [2, 8, 2, 2048, 384], P('pipe', 'expert', None, 'dp'), may hold values from -60 to 60
- outer_mean: bfloat16 [2, 8, 384, 2048], P('pipe', 'expert', None, 'dp'), may hold values from -60 to 60
- inner_square: bfloat16 [2, 8, 2, 2048, 384], P('pipe', 'expert', None, 'dp'), may hold values from 10 to 1000
- outer_square: bfloat16 [2, 8, 384, 2048], P('pipe', 'expert', None, 'dp'), may hold values from 10 to 1000
Outputs:
- layer_out: bfloat16 [2, 2048, 2048], P('pipe', ('expert', 'dp'))
- weight_inner: float32 [2, 8, 2, 2048, 384], P('pipe', 'expert', None, 'dp')
- weight_outer: float32 [2, 8, 384, 2048], P('pipe', 'expert', None, 'dp')
- mean_inner: bfloat16 [2, 8, 2, 2048, 384], P('pipe', 'expert', None, 'dp')
- mean_outer: bfloat16 [2, 8, 384, 2048], P('pipe', 'expert', None, 'dp')
- square_inner: bfloat16 [2, 8, 2, 2048, 384], P('pipe', 'expert', None, 'dp')
- square_outer: bfloat16 [2, 8, 384, 2048], P('pipe', 'expert', None, 'dp')
The draws below stay inside these ranges and needn't reach their ends.
Inputs may be any that keep to these rules, and one draw needn't show every extreme that they name: `first_ids`: each token names 2 different experts. Within the rows of one device no expert is named more than 72 times, and some device names some expert exactly 72 times. `second_ids`: as first_ids. `new_slot`: for each section, a permutation of the 4 experts.
All inputs are finite; a program needn't handle non-finite values.
Results may differ from the reference program's by a relative error of at most 0.008.
Values may be sent and summed in bfloat16 or wider, within the bound.
A program may use at most 128 MiB of HBM per device.

```python
import math
import jax
import jax.numpy as jnp
import numpy as np
from jax import lax

D = 2048
FF = 768
TOK_DEV = 128
EXPERTS = 4
TOPK = 2
CAP = 72
TOKENS = 2048
N_PIPE = 2
N_EXPERT = 8
N_DP = 2


def shard_levels(stream_key, extent, shards, least, largest):
    loudness, own = 1.0, jax.random.fold_in(stream_key, 6)
    for dim, shards_of in shards:
        draws = jnp.exp(jax.random.uniform(jax.random.fold_in(own, dim), (shards_of,), jnp.float32, least / len(shards), largest / len(shards)))
        loudness = loudness * jnp.repeat(draws, extent[dim] // shards_of).reshape([-1 if axis == dim else 1 for axis in range(len(extent))])
    return loudness


def routed_block(key, own, number, rows, count, top, reach, lean):
    sequence = jax.random.permutation(key, count)
    packed, ordinary = load_shares(count, rows * top, reach, lean, True), load_shares(count, rows * top, reach, lean, False)
    places = jnp.arange(count)

    def named(lengths, offset_by):
        used = int((lengths > 0).sum())
        fixed = max(1, used // 4)
        passed = fixed + (places - fixed + offset_by * (used - fixed)) % max(1, count - fixed)
        return jnp.zeros((count,), jnp.int32).at[sequence[jnp.where(places < fixed, places, passed)]].set(jnp.asarray(lengths, jnp.int32))

    lengths = jnp.where(number % 4 == 0, named(packed, number // 4), named(ordinary, number - number // 4 - 1))
    mixed = jax.random.permutation(jax.random.fold_in(own, 3), count)
    source_of, sink = mixed[0:count // 2 * 2:2], mixed[1:count // 2 * 2:2]
    margin = jnp.minimum(lengths[source_of] - 1, reach - lengths[sink]) // 2
    margin = jnp.where((source_of == sequence[0]) | (sink == sequence[0]) | (lengths[sink] == 0), 0, jnp.maximum(margin, 0))
    passed = jax.random.randint(jax.random.fold_in(own, 4), (count // 2,), 0, 1 << 20) % (margin + 1)
    lengths = lengths.at[source_of].add(-passed).at[sink].add(passed)
    items = jnp.searchsorted(jnp.cumsum(lengths), jnp.arange(rows * top), side="right").astype(jnp.int32)
    listing = items.reshape(top, rows).T
    listing = listing[jax.random.permutation(jax.random.fold_in(own, 1), rows)]
    offset_by = jax.random.randint(jax.random.fold_in(own, 2), (rows, 1), 0, top)
    return jnp.take_along_axis(listing, (jnp.arange(top)[None, :] + offset_by) % top, axis=1)


def load_shares(amount, total, bound, lean, full):
    portions = [(1 << 20) // math.isqrt(grade ** lean) + 1 for grade in range(1, amount + 1)]
    largest = bound if full else min(bound, max(-(-total // amount), total * portions[0] // sum(portions)))
    least = 1 if total - largest >= amount - 1 else 0
    given, rest = [largest] + [least] * (amount - 1), total - largest - least * (amount - 1)
    while rest > 0:
        movable = [i for i in range(1, amount) if given[i] < largest] or [i for i in range(1, amount) if given[i] < bound]
        mass, left = sum([portions[i] for i in movable]), rest
        for i in movable:
            more = min(bound - given[i], max(1, left * portions[i] // mass), rest)
            given[i] = given[i] + more
            rest = rest - more
    return np.array(given)


def centred(rng, extent, spread, bound, shards=(), held_as=jnp.bfloat16):
    entries = spread * jax.random.normal(rng, extent, jnp.float32)
    if shards:
        entries = entries * shard_levels(rng, extent, shards, -0.22, 0.18)
    return jnp.clip(entries, -bound, bound).astype(held_as)


def setup_inputs(seed: int = 0) -> dict:
    arg_keys = jax.random.split(jax.random.key(seed), 15)
    tokens = centred(arg_keys[0], (N_PIPE, TOKENS, D), 1.0, 6.0, ((0, 2), (1, 16)))
    cotangent = centred(arg_keys[1], (N_PIPE, TOKENS, D), 1.0, 6.0, ((0, 2), (1, 16)))
    norm_gain = jnp.clip(1.0 + 0.1 * jax.random.normal(arg_keys[2], (N_PIPE, D), jnp.float32), 0.5, 1.5)
    first_ids_keys = jax.random.split(jax.random.fold_in(arg_keys[3], 1), N_PIPE * TOKENS // TOK_DEV)
    first_ids_turns = jax.random.permutation(jax.random.fold_in(arg_keys[3], 3), N_PIPE * TOKENS // TOK_DEV)
    first_ids = jax.vmap(lambda own, number: routed_block(jax.random.fold_in(arg_keys[3], 2), own, number, TOK_DEV, EXPERTS, TOPK, CAP, 1))(first_ids_keys, first_ids_turns).reshape((N_PIPE, TOKENS, TOPK))
    first_gates = jnp.clip(0.1 + 0.9 * jax.random.uniform(arg_keys[4], (N_PIPE, TOKENS, TOPK), jnp.float32) ** shard_levels(arg_keys[4], (N_PIPE, TOKENS, TOPK), ((0, 2), (1, 16)), -0.2, 0.2), 0.1, 1.0)
    second_ids_keys = jax.random.split(jax.random.fold_in(arg_keys[5], 1), N_PIPE * TOKENS // TOK_DEV)
    second_ids_turns = jax.random.permutation(jax.random.fold_in(arg_keys[5], 3), N_PIPE * TOKENS // TOK_DEV)
    second_ids = jax.vmap(lambda own, number: routed_block(jax.random.fold_in(arg_keys[5], 2), own, number, TOK_DEV, EXPERTS, TOPK, CAP, 1))(second_ids_keys, second_ids_turns).reshape((N_PIPE, TOKENS, TOPK))
    second_gates = jnp.clip(0.1 + 0.9 * jax.random.uniform(arg_keys[6], (N_PIPE, TOKENS, TOPK), jnp.float32) ** shard_levels(arg_keys[6], (N_PIPE, TOKENS, TOPK), ((0, 2), (1, 16)), -0.2, 0.2), 0.1, 1.0)
    new_slot = jax.vmap(lambda own: jax.random.permutation(own, EXPERTS))(jax.random.split(arg_keys[7], N_PIPE)).reshape((N_PIPE, EXPERTS)).astype(jnp.int32)
    inner_weight = centred(arg_keys[8], (N_PIPE, 2 * EXPERTS, 2, D, FF // 2), D ** -0.5, 0.125, ((0, 2), (1, 8), (3, 2)), jnp.float32)
    outer_weight = centred(arg_keys[9], (N_PIPE, 2 * EXPERTS, FF // 2, D), FF ** -0.5, 0.21875, ((0, 2), (1, 8), (3, 2)), jnp.float32)
    inner_mean = centred(arg_keys[10], (N_PIPE, 2 * EXPERTS, 2, D, FF // 2), 10.0, 60.0, ((0, 2), (1, 8), (3, 2)))
    outer_mean = centred(arg_keys[11], (N_PIPE, 2 * EXPERTS, FF // 2, D), 10.0, 60.0, ((0, 2), (1, 8), (3, 2)))
    inner_square = jnp.clip(jnp.exp(math.log(1000.0) - 4.6051702 * jax.random.uniform(arg_keys[12], (N_PIPE, 2 * EXPERTS, 2, D, FF // 2), jnp.float32) ** shard_levels(arg_keys[12], (N_PIPE, 2 * EXPERTS, 2, D, FF // 2), ((0, 2), (1, 8), (3, 2)), -0.2, 0.2)), 10.0, 1000.0).astype(jnp.bfloat16)
    outer_square = jnp.clip(jnp.exp(math.log(1000.0) - 4.6051702 * jax.random.uniform(arg_keys[13], (N_PIPE, 2 * EXPERTS, FF // 2, D), jnp.float32) ** shard_levels(arg_keys[13], (N_PIPE, 2 * EXPERTS, FF // 2, D), ((0, 2), (1, 8), (3, 2)), -0.2, 0.2)), 10.0, 1000.0).astype(jnp.bfloat16)
    return {"tokens": tokens, "cotangent": cotangent, "norm_gain": norm_gain, "first_ids": first_ids, "first_gates": first_gates, "second_ids": second_ids, "second_gates": second_gates, "new_slot": new_slot, "inner_weight": inner_weight, "outer_weight": outer_weight, "inner_mean": inner_mean, "outer_mean": outer_mean, "inner_square": inner_square, "outer_square": outer_square}


norm_eps = 1e-06
learn_rate = 0.001
beta_one = 0.9
beta_two = 0.95
adam_eps = 1e-08
bias_one = 0.999973438601112
bias_two = 0.994079470779667

def normed(values, gain_row):
    widened = values.astype(jnp.float32)
    inverse_rms = lax.rsqrt(lax.optimization_barrier(jnp.mean(widened * widened, axis=-1, keepdims=True)) + norm_eps)
    return (widened * inverse_rms * gain_row).astype(jnp.bfloat16)

def silu_parts(gate_proj):
    logistic = jax.nn.sigmoid(gate_proj)
    return (gate_proj * logistic, logistic * (1.0 + gate_proj * (1.0 - logistic)))

def half_forward(token_rows, inner_full, outer_full):
    gate_proj = jnp.dot(token_rows, inner_full[0], preferred_element_type=jnp.float32)
    up_proj = jnp.dot(token_rows, inner_full[1], preferred_element_type=jnp.float32)
    activity = (silu_parts(gate_proj)[0] * up_proj).astype(jnp.bfloat16)
    half_out = jnp.dot(activity, outer_full, preferred_element_type=jnp.float32).astype(jnp.bfloat16)
    return (half_out, activity, gate_proj, up_proj)

def half_backward(token_rows, grad_rows, outer_full, activity, gate_proj, up_proj):
    grad_outer = jnp.dot(activity.T, grad_rows, preferred_element_type=jnp.float32)
    d_active = jnp.dot(grad_rows, outer_full.T, preferred_element_type=jnp.float32)
    swish_value, swish_slope = silu_parts(gate_proj)
    d_gate = (d_active * up_proj * swish_slope).astype(jnp.bfloat16)
    d_upper = (d_active * swish_value).astype(jnp.bfloat16)
    grad_gate = jnp.dot(token_rows.T, d_gate, preferred_element_type=jnp.float32)
    grad_upper = jnp.dot(token_rows.T, d_upper, preferred_element_type=jnp.float32)
    return (jnp.stack([grad_gate, grad_upper]), grad_outer)

def slot_rows(ids):
    blocked = ids.reshape(-1, TOK_DEV * TOPK)
    onehot = (blocked[..., None] == jnp.arange(EXPERTS, dtype=jnp.int32)).astype(jnp.int32)
    ranking = lax.optimization_barrier(jnp.sum((jnp.cumsum(onehot, axis=1) - 1) * onehot, axis=2)).astype(jnp.int32)
    starts = jnp.arange(blocked.shape[0], dtype=jnp.int32)[:, None] * CAP
    return (starts + ranking).reshape(ids.shape).astype(jnp.int32)

def scatter_rows(values, ids, positions):
    buffer = jnp.zeros((EXPERTS, TOKENS // TOK_DEV * CAP, D), jnp.bfloat16)
    return buffer.at[ids, positions].set(values)

def section_forward(token_rows, gain_row, ids, gates, inner_low, outer_low):
    normal = normed(token_rows, gain_row)
    positions = slot_rows(ids)
    buffer = scatter_rows(jnp.broadcast_to(normal[:, None, :], ids.shape + (D,)), ids, positions)
    totals = []
    stored = []
    for expert in range(EXPERTS):
        summed = jnp.zeros((buffer.shape[1], D), jnp.float32)
        for half_index in range(2):
            slot = 2 * expert + half_index
            half_out, activity, gate_proj, up_proj = half_forward(buffer[expert], inner_low[slot], outer_low[slot])
            summed = summed + lax.optimization_barrier(half_out).astype(jnp.float32)
            stored.append((activity, gate_proj, up_proj))
        totals.append(summed)
    totals = jnp.stack(totals)
    picked = totals[ids, positions]
    mixed_rows = token_rows.astype(jnp.float32) + lax.optimization_barrier(jnp.sum(gates[..., None] * picked, axis=1))
    return (mixed_rows.astype(jnp.bfloat16), buffer, stored)

def group_rows(values, dp_group):
    return values.reshape(N_EXPERT, N_DP, CAP, values.shape[-1])[:, dp_group].reshape(-1, values.shape[-1])

def section_grads(buffer, stored, grad_out, ids, gates, outer_low):
    positions = slot_rows(ids)
    grad_rows = (gates[..., None] * grad_out.astype(jnp.float32)[:, None, :]).astype(jnp.bfloat16)
    grad_buffer = scatter_rows(grad_rows, ids, positions)
    inner_list = []
    outer_list = []
    for expert in range(EXPERTS):
        for half_index in range(2):
            slot = 2 * expert + half_index
            activity, gate_proj, up_proj = stored[slot]
            total_inner = jnp.zeros((2, D, FF // 2), jnp.float32)
            total_outer = jnp.zeros((FF // 2, D), jnp.float32)
            for dp_group in range(N_DP):
                grad_inner, grad_outer = half_backward(group_rows(buffer[expert], dp_group), group_rows(grad_buffer[expert], dp_group), outer_low[slot], group_rows(activity, dp_group), group_rows(gate_proj, dp_group), group_rows(up_proj, dp_group))
                total_inner = total_inner + lax.optimization_barrier(grad_inner.astype(jnp.bfloat16)).astype(jnp.float32)
                total_outer = total_outer + lax.optimization_barrier(grad_outer.astype(jnp.bfloat16)).astype(jnp.float32)
            inner_list.append(total_inner)
            outer_list.append(total_outer)
    return (jnp.stack(inner_list), jnp.stack(outer_list))

def adam_step(weight, mean, square, grads):
    mean_new = (beta_one * mean.astype(jnp.float32) + (1.0 - beta_one) * grads).astype(jnp.bfloat16)
    square_new = (beta_two * square.astype(jnp.float32) + (1.0 - beta_two) * grads * grads).astype(jnp.bfloat16)
    mean_wide = lax.optimization_barrier(mean_new).astype(jnp.float32)
    square_wide = lax.optimization_barrier(square_new).astype(jnp.float32)
    update = mean_wide / bias_one / (jnp.sqrt(square_wide / bias_two) + adam_eps)
    return (weight - learn_rate * update, mean_new, square_new)

def reference(tokens, cotangent, norm_gain, first_ids, first_gates, second_ids, second_gates, new_slot, inner_weight, outer_weight, inner_mean, outer_mean, inner_square, outer_square):
    first_list = []
    inner_grads = []
    outer_grads = []
    for section in range(N_PIPE):
        inner_low = inner_weight[section].astype(jnp.bfloat16)
        outer_low = outer_weight[section].astype(jnp.bfloat16)
        section_out, buffer, stored = section_forward(tokens[section], norm_gain[section], first_ids[section], first_gates[section], inner_low, outer_low)
        grad_inner, grad_outer = section_grads(buffer, stored, cotangent[section], first_ids[section], first_gates[section], outer_low)
        first_list.append(section_out)
        inner_grads.append(grad_inner)
        outer_grads.append(grad_outer)
    first_out = lax.optimization_barrier(jnp.stack(first_list))
    second_in = jnp.roll(first_out, 1, axis=0)
    inner_new, inner_mean_new, inner_square_new = adam_step(inner_weight, inner_mean, inner_square, jnp.stack(inner_grads))
    outer_new, outer_mean_new, outer_square_new = adam_step(outer_weight, outer_mean, outer_square, jnp.stack(outer_grads))
    second_list = []
    for section in range(N_PIPE):
        section_out, buffer, stored = section_forward(second_in[section], norm_gain[section], second_ids[section], second_gates[section], inner_new[section].astype(jnp.bfloat16), outer_new[section].astype(jnp.bfloat16))
        second_list.append(section_out)
    layer_out = jnp.stack(second_list)
    sources = []
    halves = jnp.arange(2 * EXPERTS, dtype=jnp.int32)
    for section in range(N_PIPE):
        inverse = jnp.zeros((EXPERTS,), jnp.int32).at[new_slot[section]].set(jnp.arange(EXPERTS, dtype=jnp.int32))
        sources.append((2 * inverse[halves // 2] + halves % 2).astype(jnp.int32))

    def placed(array):
        return jnp.stack([array[section][sources[section]] for section in range(N_PIPE)])
    return (layer_out, placed(inner_new), placed(outer_new), placed(inner_mean_new), placed(outer_mean_new), placed(inner_square_new), placed(outer_square_new))
```

```python
import jax
import jax.numpy as jnp
from jax import lax
from jax.sharding import PartitionSpec as P

norm_eps = 1e-06
learn_rate = 0.001
beta_one = 0.9
beta_two = 0.95
adam_eps = 1e-08
bias_one = 0.999973438601112
bias_two = 0.994079470779667


def for_sending(array):

    def short(part):
        return part.astype(jnp.bfloat16) if part.dtype == jnp.float32 else part

    return jax.tree.map(short, array)


def passed_along(block, axis, distance):
    devices = range(lax.axis_size(axis))
    route = [((i - distance) % len(devices), i) for i in devices]
    return lax.ppermute(block, axis, route)


def normed(values, gain_row):
    widened = values.astype(jnp.float32)
    inverse_rms = lax.rsqrt(jnp.mean(widened * widened, axis=-1, keepdims=True) + norm_eps)
    return (widened * inverse_rms * gain_row).astype(jnp.bfloat16)


def silu_parts(gate_proj):
    logistic = jax.nn.sigmoid(gate_proj)
    return (gate_proj * logistic, logistic * (1.0 + gate_proj * (1.0 - logistic)))


def half_forward(token_rows, inner_full, outer_full):
    gate_proj = jnp.dot(token_rows, inner_full[0], preferred_element_type=jnp.float32)
    up_proj = jnp.dot(token_rows, inner_full[1], preferred_element_type=jnp.float32)
    activity = (silu_parts(gate_proj)[0] * up_proj).astype(jnp.bfloat16)
    half_out = jnp.dot(activity, outer_full, preferred_element_type=jnp.float32).astype(
        jnp.bfloat16
    )
    return (half_out, activity, gate_proj, up_proj)


def half_backward(token_rows, grad_rows, outer_full, activity, gate_proj, up_proj):
    grad_outer = jnp.dot(activity.T, grad_rows, preferred_element_type=jnp.float32)
    d_active = jnp.dot(grad_rows, outer_full.T, preferred_element_type=jnp.float32)
    swish_value, swish_slope = silu_parts(gate_proj)
    d_gate = (d_active * up_proj * swish_slope).astype(jnp.bfloat16)
    d_upper = (d_active * swish_value).astype(jnp.bfloat16)
    grad_gate = jnp.dot(token_rows.T, d_gate, preferred_element_type=jnp.float32)
    grad_upper = jnp.dot(token_rows.T, d_upper, preferred_element_type=jnp.float32)
    return (jnp.stack([grad_gate, grad_upper]), grad_outer)


def slot_index(ids, pair_of, capacity):
    flattened = ids.reshape(-1)
    expert_row = jnp.arange(pair_of.shape[0], dtype=jnp.int32)
    onehot = (flattened[:, None] == expert_row[None, :]).astype(jnp.int32)
    ranking = jnp.sum((jnp.cumsum(onehot, axis=0) - 1) * onehot, axis=1)
    target = jnp.sum(onehot * pair_of[None, :], axis=1)
    return (target * capacity + ranking).reshape(ids.shape)


def selection(slots, values, total_slots):
    positions = jnp.arange(total_slots, dtype=jnp.int32)
    result = jnp.zeros((total_slots, slots.shape[0]), jnp.float32)
    for column in range(slots.shape[1]):
        result = result + jnp.where(
            slots[:, column][None, :] == positions[:, None], values[:, column][None, :], 0.0
        )
    return result


def across_chips(blocks):
    pairs = blocks.shape[0]
    groups = [[2 * pair + core for pair in range(pairs)] for core in range(2)]
    return lax.all_to_all(
        blocks, "expert", split_axis=0, concat_axis=0, tiled=True, axis_index_groups=groups
    )


def to_partner(block):
    devices = range(lax.axis_size("expert"))
    return lax.ppermute(block, "expert", [(i, i ^ 1) for i in devices])


def dispatched(packed, pair_count, capacity):
    own = across_chips(packed.reshape(pair_count, capacity, packed.shape[-1]))
    own = own.reshape(pair_count * capacity, -1)
    return jnp.concatenate([own, to_partner(own)], axis=0)


def gather_weights(inner_master, outer_master):
    inner_full, outer_full = (
        lax.all_gather(inner_master.astype(jnp.bfloat16), "dp", axis=3, tiled=True),
        lax.all_gather(outer_master.astype(jnp.bfloat16), "dp", axis=3, tiled=True),
    )
    return (inner_full[0, 0], outer_full[0, 0])


def pack_rows(token_rows, gain_row, ids, pair_of, capacity):
    pair_count = pair_of.shape[0]
    normal = normed(token_rows, gain_row)
    slots = slot_index(ids, pair_of, capacity)
    picker = selection(slots, jnp.ones(slots.shape, jnp.float32), pair_count * capacity).astype(
        jnp.bfloat16
    )
    packed = jnp.dot(picker, normal, preferred_element_type=jnp.float32).astype(jnp.bfloat16)
    return (slots, dispatched(packed, pair_count, capacity))


def returned_rows(token_rows, half_out, slots, gates, pair_count, capacity):
    rows = pair_count * capacity
    summed = half_out[:rows].astype(jnp.float32) + to_partner(half_out[rows:]).astype(jnp.float32)
    back = across_chips(summed.astype(jnp.bfloat16).reshape(pair_count, capacity, -1))
    weighting = selection(slots, gates, rows)
    mixed = lax.dot_general(
        weighting,
        back.reshape(rows, -1).astype(jnp.float32),
        (((0,), (0,)), ((), ())),
        precision=lax.Precision.HIGHEST,
    )
    return (token_rows.astype(jnp.float32) + mixed).astype(jnp.bfloat16)


def adam_step(weight, mean, square, grads):
    mean_new = (beta_one * mean.astype(jnp.float32) + (1.0 - beta_one) * grads).astype(jnp.bfloat16)
    square_new = (beta_two * square.astype(jnp.float32) + (1.0 - beta_two) * grads * grads).astype(
        jnp.bfloat16
    )
    mean_wide = lax.optimization_barrier(mean_new).astype(jnp.float32)
    square_wide = lax.optimization_barrier(square_new).astype(jnp.float32)
    update = mean_wide / bias_one / (jnp.sqrt(square_wide / bias_two) + adam_eps)
    return (weight - learn_rate * update, mean_new, square_new)


def relocated(inner, outer, source):
    devices = source.shape[0]

    def moved(parts):
        spread = lax.all_to_all(parts, "expert", split_axis=0, concat_axis=0, tiled=True)
        ordered = jnp.take(spread, source, axis=0)
        return lax.all_to_all(ordered, "expert", split_axis=0, concat_axis=0, tiled=True)

    two, rows, columns = inner.shape[2:]
    parts = inner.reshape(two, devices, rows // devices, columns).transpose(1, 0, 2, 3)
    inner_back = moved(parts).transpose(1, 0, 2, 3).reshape(inner.shape)
    parts = outer.reshape(devices, outer.shape[2] // devices, outer.shape[3])
    return (inner_back, moved(parts).reshape(outer.shape))


def per_device(
    tokens,
    cotangent,
    norm_gain,
    first_ids,
    first_gates,
    second_ids,
    second_gates,
    new_slot,
    inner_weight,
    outer_weight,
    inner_mean,
    outer_mean,
    inner_square,
    outer_square,
):
    pair_count = new_slot.shape[1]
    rows_here = tokens.shape[1]
    top_count = first_ids.shape[2]
    width = tokens.shape[2]
    usual = rows_here * top_count // pair_count
    capacity = min(rows_here, usual + usual // 8)
    gain_row = norm_gain[0]
    identity_map = jnp.arange(pair_count, dtype=jnp.int32)
    new_pairs = new_slot[0]
    inverse = jnp.sum(
        jnp.where(new_pairs[:, None] == identity_map[None, :], identity_map[:, None], 0), axis=0
    )
    device_ids = jnp.arange(2 * pair_count, dtype=jnp.int32)
    source = 2 * jnp.repeat(inverse, 2) + device_ids % 2
    inner_low, outer_low = relocated(*for_sending((inner_weight, outer_weight)), source)
    inner_full, outer_full = gather_weights(inner_low, outer_low)
    slots, arrived = pack_rows(tokens[0], gain_row, first_ids[0], new_pairs, capacity)
    weighting = selection(slots, first_gates[0], pair_count * capacity)
    grad_packed = jnp.dot(
        weighting, cotangent[0].astype(jnp.float32), precision=lax.Precision.HIGHEST
    ).astype(jnp.bfloat16)
    grad_arrived = dispatched(grad_packed, pair_count, capacity)
    moments = (inner_mean, outer_mean, inner_square, outer_square)
    moments, inner_low, outer_low = lax.optimization_barrier((moments, inner_low, outer_low))
    old_mean_in, old_mean_out = relocated(moments[0], moments[1], source)
    old_square_in, old_square_out = relocated(moments[2], moments[3], source)
    half_out, activity, gate_proj, up_proj = half_forward(arrived, inner_full, outer_full)
    grad_inner, grad_outer = half_backward(
        arrived, grad_arrived, outer_full, activity, gate_proj, up_proj
    )
    sum_inner, sum_outer = (
        lax.psum_scatter(
            grad_inner[None, None].astype(jnp.bfloat16), "dp", scatter_dimension=3, tiled=True
        ).astype(jnp.float32),
        lax.psum_scatter(
            grad_outer[None, None].astype(jnp.bfloat16), "dp", scatter_dimension=3, tiled=True
        ).astype(jnp.float32),
    )
    first_out = returned_rows(
        tokens[0], half_out, slots, first_gates[0], pair_count, capacity
    )
    moved_inner, moved_mean_in, moved_square_in = adam_step(
        inner_low.astype(jnp.float32), old_mean_in, old_square_in, sum_inner
    )
    moved_outer, moved_mean_out, moved_square_out = adam_step(
        outer_low.astype(jnp.float32), old_mean_out, old_square_out, sum_outer
    )
    inner_two, outer_two = gather_weights(moved_inner, moved_outer)
    shifted = passed_along(first_out, "pipe", 1)
    slots_two, arrived_two = pack_rows(shifted, gain_row, second_ids[0], new_pairs, capacity)
    half_two = half_forward(arrived_two, inner_two, outer_two)[0]
    second_out = returned_rows(
        shifted, half_two, slots_two, second_gates[0], pair_count, capacity
    )
    return (
        second_out[None],
        moved_inner,
        moved_outer,
        moved_mean_in,
        moved_mean_out,
        moved_square_in,
        moved_square_out,
    )


def solution(mesh):
    return jax.shard_map(
        per_device,
        mesh=mesh,
        in_specs=(
            P("pipe", ("expert", "dp"), None),
            P("pipe", ("expert", "dp"), None),
            P("pipe", None),
            P("pipe", ("expert", "dp"), None),
            P("pipe", ("expert", "dp"), None),
            P("pipe", ("expert", "dp"), None),
            P("pipe", ("expert", "dp"), None),
            P("pipe", None),
            P("pipe", "expert", None, "dp", None),
            P("pipe", "expert", None, "dp"),
            P("pipe", "expert", None, "dp", None),
            P("pipe", "expert", None, "dp"),
            P("pipe", "expert", None, "dp", None),
            P("pipe", "expert", None, "dp"),
        ),
        out_specs=(
            P("pipe", ("expert", "dp"), None),
            P("pipe", "expert", None, "dp", None),
            P("pipe", "expert", None, "dp"),
            P("pipe", "expert", None, "dp", None),
            P("pipe", "expert", None, "dp"),
            P("pipe", "expert", None, "dp", None),
            P("pipe", "expert", None, "dp"),
        ),
        check_vma=False,
    )
```
